32 devices in a mesh: fsdp: 16 (over z, x, core), tensor: 2 (over y).
Axes of the slice: x: 2, y: 2, z: 4, core: 2. Of those that a mesh axis runs over, the one named last changes fastest.
Arguments:
- tokens: bfloat16 [6144, 2048], P(('fsdp', 'tensor')), may hold values from -6 to 6
- segment_ids: int32 [16, 384], P('fsdp'), may hold values from 0 to 2, never falling along the last dimension, each value on 1 to 192 neighbouring positions
- w_query: bfloat16 [2048, 2048], P('fsdp', 'tensor'), may hold values from -0.125 to 0.125
- w_key: bfloat16 [2048, 2048], P('fsdp', 'tensor'), may hold values from -0.125 to 0.125
- w_value: bfloat16 [2048, 2048], P('fsdp', 'tensor'), may hold values from -0.125 to 0.125
- w_out: bfloat16 [2048, 2048], P('tensor', 'fsdp'), may hold values from -0.125 to 0.125
- w_gate: bfloat16 [2048, 8192], P('fsdp', 'tensor'), may hold values from -0.125 to 0.125
- w_up: bfloat16 [2048, 8192], P('fsdp', 'tensor'), may hold values from -0.125 to 0.125
- w_down: bfloat16 [8192, 2048], P('tensor', 'fsdp'), may hold values from -0.0625 to 0.0625
- gain_query: bfloat16 [2048], P('fsdp'), may hold values from 0.25 to 1.75
- gain_key: bfloat16 [2048], P('fsdp'), may hold values from 0.25 to 1.75
- gain_attn: bfloat16 [2048], P('fsdp'), may hold values from 0.25 to 1.75
- gain_ffn: bfloat16 [2048], P('fsdp'), may hold values from 0.25 to 1.75
- cotangent: bfloat16 [6144, 2048], P(('fsdp', 'tensor')), may hold values from -6 to 6
Outputs:
- layer_out: bfloat16 [6144, 2048], P(('fsdp', 'tensor'))
- grad_tokens: float32 [6144, 2048], P(('fsdp', 'tensor'))
- grad_w_query: float32 [2048, 2048], P('fsdp', 'tensor')
- grad_w_key: float32 [2048, 2048], P('fsdp', 'tensor')
- grad_w_value: float32 [2048, 2048], P('fsdp', 'tensor')
- grad_w_out: float32 [2048, 2048], P('tensor', 'fsdp')
- grad_w_gate: float32 [2048, 8192], P('fsdp', 'tensor')
- grad_w_up: float32 [2048, 8192], P('fsdp', 'tensor')
- grad_w_down: float32 [8192, 2048], P('tensor', 'fsdp')
- grad_gain_query: float32 [2048], P('fsdp')
- grad_gain_key: float32 [2048], P('fsdp')
- grad_gain_attn: float32 [2048], P('fsdp')
- grad_gain_ffn: float32 [2048], P('fsdp')
The draws below stay inside these ranges and needn't reach their ends.
Inputs may be any that keep to these rules, and one draw needn't show every extreme that they name: `segment_ids`: in each row, ids never fall; each of the 3 ids covers 1 to 192 positions, and one covers exactly 192.
All inputs are finite; a program needn't handle non-finite values.
Results may differ from the reference program's by a relative error of at most 0.015.
Values may be sent and summed in bfloat16 or wider, within the bound.
A program may use at most 256 MiB of HBM per device.

```python
import math
import jax
import jax.numpy as jnp
import numpy as np
from jax import lax

D = 2048
HEADS = 16
HEAD_DIM = 128
FF = 8192
DOCS = 3
SEQ = 384
TOKENS = 6144
N_FSDP = 16


def spiked(array, rng, source, target, shards_of, factor):
    def block_of(dim):
        return (jnp.arange(array.shape[dim]) // (array.shape[dim] // shards_of)).reshape((-1,) + (1,) * (array.ndim - 1 - dim))

    first = jax.random.permutation(rng, shards_of)[block_of(target)]
    far = (block_of(target) + shards_of // 2) % shards_of
    return jnp.where((block_of(source) == first) | (block_of(source) == far), factor * array, array)


def levels(rng, shape, cuts, smallest, high):
    level, own = 1.0, jax.random.fold_in(rng, 6)
    for dim, shards_of in cuts:
        heights = jnp.exp(jax.random.uniform(jax.random.fold_in(own, dim), (shards_of,), jnp.float32, smallest / len(cuts), high / len(cuts)))
        level = level * jnp.repeat(heights, shape[dim] // shards_of).reshape([-1 if axis == dim else 1 for axis in range(len(shape))])
    return level


def split_up(number_of, total, most, lean):
    weights = [(1 << 20) // math.isqrt(standing ** lean) + 1 for standing in range(2, number_of + 1)]
    spare, holding = total - most - (number_of - 1), [1] * (number_of - 1)
    while spare > 0:
        candidates = [i for i in range(number_of - 1) if holding[i] < most]
        whole, left = sum([weights[i] for i in candidates]), spare
        for i in candidates:
            addition = min(most - holding[i], max(1, left * weights[i] // whole), spare)
            holding[i] = holding[i] + addition
            spare = spare - addition
    return np.array([most] + holding)


def ragged_sizes(key, count, total, limit, skew):
    if count == 2:
        one = jax.random.randint(key, (), max(1, total - limit), min(limit, total - 1) + 1)
        return jnp.stack([one, total - one])
    sizes = jnp.asarray(split_up(count, total, limit, skew), jnp.int32)
    twos = (count - 1) // 2
    donor, sink = sizes[1:1 + 2 * twos:2], sizes[2:2 + 2 * twos:2]
    slack = jnp.minimum(donor - 1, limit - sink)
    moved = jax.random.randint(jax.random.fold_in(key, 1), (twos,), 0, 1 << 20) % (slack + 1)
    sizes = sizes.at[1:1 + 2 * twos:2].set(donor - moved).at[2:2 + 2 * twos:2].set(sink + moved)
    return sizes[jax.random.permutation(jax.random.fold_in(key, 2), count)]


def scatter_about(stream_key, dims, spread, reach, pieces=(), held_as=jnp.bfloat16):
    drawn = jax.random.normal(stream_key, dims, jnp.float32) * spread
    if len(pieces) > 0:
        drawn = levels(stream_key, dims, pieces, -0.22, 0.18) * drawn
    return jnp.clip(drawn, min=-reach, max=reach).astype(held_as)


def gaussian_with(own_key, extent, width, bound, shards, heavy, kind=jnp.bfloat16):
    drawn = width * jax.random.normal(own_key, extent, jnp.float32)
    if shards:
        drawn = drawn * levels(own_key, extent, shards, -0.22, 0.18)
    return jnp.clip(spiked(drawn, jax.random.fold_in(own_key, 3), *heavy), -bound, bound).astype(kind)


def setup_inputs(seed: int = 0) -> dict:
    keys = jax.random.split(jax.random.key(seed), 15)
    tokens = gaussian_with(keys[0], (TOKENS, D), 1.0, 6.0, ((0, 32),), (0, 1, 32, 2.75))
    segment_ids = jax.vmap(lambda own: jnp.searchsorted(jnp.cumsum(ragged_sizes(own, DOCS, SEQ, SEQ // 2, 0)), jnp.arange(SEQ), side="right"))(jax.random.split(keys[1], N_FSDP)).reshape((N_FSDP, SEQ)).astype(jnp.int32)
    w_query = scatter_about(keys[2], (D, D), D ** -0.5, 0.125, ((0, 16), (1, 2)))
    w_key = scatter_about(keys[3], (D, D), D ** -0.5, 0.125, ((0, 16), (1, 2)))
    w_value = scatter_about(keys[4], (D, D), D ** -0.5, 0.125, ((0, 16), (1, 2)))
    w_out = scatter_about(keys[5], (D, D), D ** -0.5, 0.125, ((0, 2), (1, 16)))
    w_gate = scatter_about(keys[6], (D, FF), D ** -0.5, 0.125, ((0, 16), (1, 2)))
    w_up = scatter_about(keys[7], (D, FF), D ** -0.5, 0.125, ((0, 16), (1, 2)))
    w_down = scatter_about(keys[8], (FF, D), FF ** -0.5, 0.0625, ((0, 2), (1, 16)))
    gain_query = jnp.clip(1.0 + 0.15 * jax.random.normal(keys[9], (D,), jnp.float32), 0.25, 1.75).astype(jnp.bfloat16)
    gain_key = jnp.clip(1.0 + 0.15 * jax.random.normal(keys[10], (D,), jnp.float32), 0.25, 1.75).astype(jnp.bfloat16)
    gain_attn = jnp.clip(1.0 + 0.15 * jax.random.normal(keys[11], (D,), jnp.float32), 0.25, 1.75).astype(jnp.bfloat16)
    gain_ffn = jnp.clip(1.0 + 0.15 * jax.random.normal(keys[12], (D,), jnp.float32), 0.25, 1.75).astype(jnp.bfloat16)
    cotangent = gaussian_with(keys[13], (TOKENS, D), 1.0, 6.0, ((0, 32),), (0, 1, 32, 2.75))
    return {"tokens": tokens, "segment_ids": segment_ids, "w_query": w_query, "w_key": w_key, "w_value": w_value, "w_out": w_out, "w_gate": w_gate, "w_up": w_up, "w_down": w_down, "gain_query": gain_query, "gain_key": gain_key, "gain_attn": gain_attn, "gain_ffn": gain_ffn, "cotangent": cotangent}


@jax.custom_vjp
def low(v):
    return lax.optimization_barrier(v.astype(jnp.bfloat16)).astype(jnp.float32)

@jax.custom_vjp
def low_back(v):
    return v

def low_keep(v):
    return (low(v), None)

def low_pass(kept, grad):
    return (grad,)

def back_keep(v):
    return (v, None)

def back_low(kept, grad):
    return (low(grad),)
low.defvjp(low_keep, low_pass)
low_back.defvjp(back_keep, back_low)
epsilon_norm = 1e-06
rope_theta = 500000.0
masked_score = -1e+30

def mixing(left, right):
    return jnp.dot(left, right, precision=lax.Precision.HIGHEST, preferred_element_type=jnp.float32)

def rms_scale(field, gain):
    return field * lax.rsqrt(lax.optimization_barrier(jnp.mean(field * field, axis=-1, keepdims=True)) + epsilon_norm) * gain

def doc_positions(segment_row):
    length = segment_row.shape[0]
    indices = jnp.arange(length, dtype=jnp.int32)
    change = jnp.concatenate([jnp.ones((1,), jnp.bool_), segment_row[1:] != segment_row[:-1]])
    begins = lax.cummax(jnp.where(change, indices, 0), axis=0)
    return (indices - begins).astype(jnp.int32)

def rope_tables(positions):
    halfway = HEAD_DIM // 2
    inverse = rope_theta ** (-(jnp.arange(halfway, dtype=jnp.float32) * 2.0) / HEAD_DIM)
    angles = positions.astype(jnp.float32)[:, None] * inverse[None, :]
    return (jnp.cos(angles), jnp.sin(angles))

def rotate(field, cosine, sine_table):
    halfway = field.shape[-1] // 2
    first_half = field[..., :halfway]
    second = field[..., halfway:]
    cos_wide = cosine[:, None, :]
    sin_wide = sine_table[:, None, :]
    return jnp.concatenate([first_half * cos_wide - second * sin_wide, second * cos_wide + first_half * sin_wide], axis=-1)

def layer_rows(tokens, segment_row, weights):
    w_query, w_key, w_value, w_out, w_gate, w_up, w_down, gain_query, gain_key, gain_attn, gain_ffn = weights
    length = tokens.shape[0]
    queries = low_back(mixing(tokens, w_query))
    key_rows = low_back(mixing(tokens, w_key))
    values = low(low_back(mixing(tokens, w_value)))
    cosine, sine_table = rope_tables(doc_positions(segment_row))
    queries_r = low(rotate(rms_scale(queries, gain_query).reshape(length, HEADS, HEAD_DIM), cosine, sine_table))
    keys_r = low(rotate(rms_scale(key_rows, gain_key).reshape(length, HEADS, HEAD_DIM), cosine, sine_table))
    score_scale = HEAD_DIM ** (-0.5)
    scores = low_back(jnp.einsum('qhd,khd->hqk', queries_r, keys_r, precision=lax.Precision.HIGHEST) * score_scale)
    indices = jnp.arange(length)
    allowed = (segment_row[:, None] == segment_row[None, :]) & (indices[:, None] >= indices[None, :])
    scores = jnp.where(allowed[None], scores, masked_score)
    attn_probs = low(jax.nn.softmax(scores, axis=-1))
    attended = jnp.einsum('hqk,khd->qhd', attn_probs, values.reshape(length, HEADS, HEAD_DIM), precision=lax.Precision.HIGHEST)
    attended = low(low_back(attended)).reshape(length, D)
    out_part = low_back(mixing(attended, w_out))
    middle = tokens + rms_scale(out_part, gain_attn)
    middle_low = low(middle)
    gate_pre = low_back(mixing(middle_low, w_gate))
    up_proj = low_back(mixing(middle_low, w_up))
    hidden = low(jax.nn.silu(gate_pre) * up_proj)
    down_out = low_back(mixing(hidden, w_down))
    return middle + rms_scale(down_out, gain_ffn)

def reference(tokens, segment_ids, w_query, w_key, w_value, w_out, w_gate, w_up, w_down, gain_query, gain_key, gain_attn, gain_ffn, cotangent):
    weights = tuple((weight_arg.astype(jnp.float32) for weight_arg in (w_query, w_key, w_value, w_out, w_gate, w_up, w_down, gain_query, gain_key, gain_attn, gain_ffn)))
    inputs = tokens.astype(jnp.float32).reshape(N_FSDP, SEQ, D)
    layer_saved = jax.checkpoint(layer_rows)

    def forward(inputs, weights):

        def per_sequence(paired):
            return layer_saved(paired[0], paired[1], weights)
        return lax.map(per_sequence, (inputs, segment_ids))
    outputs, pullback = jax.vjp(forward, inputs, weights)
    grad_inputs, grad_weights = pullback(cotangent.astype(jnp.float32).reshape(N_FSDP, SEQ, D))
    return (outputs.reshape(TOKENS, D).astype(jnp.bfloat16), grad_inputs.reshape(TOKENS, D), grad_weights[0], grad_weights[1], grad_weights[2], grad_weights[3], grad_weights[4], grad_weights[5], grad_weights[6], grad_weights[7], grad_weights[8], grad_weights[9], grad_weights[10])
```

```python
import functools

import jax
import jax.numpy as jnp
from jax import lax
from jax.experimental import pallas as pl
from jax.experimental.pallas import tpu as pltpu
from jax.sharding import PartitionSpec as P

HEAD_DIM = 128
epsilon_norm = 1e-06
rope_theta = 500000.0
masked_score = -1e30
MESH = pl.DeviceIdType.MESH
SWAP = [(0, 1), (1, 0)]


def ring_chip(pos, n):
    if n != 8:
        return pos
    x = pos // 4
    z = pos + x * (7 - 2 * pos)
    return z * 2 + x


def ring_pos(chip, n):
    if n != 8:
        return chip
    x = chip % 2
    z = chip // 2
    return z + x * (7 - 2 * z)


class Ring:
    def __init__(self, n):
        self.n = n
        self.h = n // 2
        self.f = lax.axis_index("fsdp")
        self.t = lax.axis_index("tensor")
        self.c = self.f % 2
        self.pos = ring_pos(self.f // 2, n)
        self.next = (self.chip(1) * 2 + self.c, self.t)
        self.prev = (self.chip(-1) * 2 + self.c, self.t)
        self.mate = (self.f + 1 - 2 * self.c, self.t)

    def chip(self, offset):
        return ring_chip((self.pos + offset + self.n) % self.n, self.n)

    def greet(self):
        barrier = pltpu.get_barrier_semaphore()
        for peer in (self.next, self.prev, self.mate):
            pl.semaphore_signal(barrier, inc=1, device_id=peer, device_id_type=MESH)
        pl.semaphore_wait(barrier, 3)


def remote(src, dst, send, recv, peer):
    return pltpu.make_async_remote_copy(
        src_ref=src,
        dst_ref=dst,
        send_sem=send,
        recv_sem=recv,
        device_id=peer,
        device_id_type=MESH,
    )


def gather_kernel(n, w_ref, g_ref, ssem, rsem, msend, mrecv, osend, orecv, lsem):
    ring = Ring(n)
    h = ring.h
    count, rows, _ = w_ref.shape
    half = rows // 2
    ring.greet()

    def slot(w, offset):
        return (ring.chip(offset) * 2 + ring.c, w)

    def part(ref, piece):
        if piece is None:
            return ref
        return ref.at[pl.ds(piece * half, half), :]

    def hop(w, way, d, piece):
        origin = -d if way == 0 else d
        s, _ = slot(w, origin)
        src = w_ref.at[w] if isinstance(d, int) and d == 0 else g_ref.at[w, s]
        return remote(
            part(src, piece),
            part(g_ref.at[w, s], piece),
            ssem.at[w, way, d % 4],
            rsem.at[w, way, d % 4],
            ring.next if way == 0 else ring.prev,
        )

    def share(w, way, d, piece):
        origin = -1 - d if way == 0 else 1 + d
        s, _ = slot(w, origin)
        ref = part(g_ref.at[w, s], piece)
        return remote(ref, ref, msend.at[w, way, d % 4], mrecv.at[w, way, d % 4], ring.mate)

    def share_in(w, way, d, piece):
        origin = -1 - d if way == 0 else 1 + d
        s = ring.chip(origin) * 2 + 1 - ring.c
        ref = part(g_ref.at[w, s], piece)
        return remote(ref, ref, msend.at[w, way, d % 4], mrecv.at[w, way, d % 4], ring.mate)

    def arrival(w, way, d, piece):
        origin = -1 - d if way == 0 else 1 + d
        s, _ = slot(w, origin)
        ref = part(g_ref.at[w, s], piece)
        return remote(
            ref,
            ref,
            ssem.at[w, way, d % 4],
            rsem.at[w, way, d % 4],
            ring.next if way == 0 else ring.prev,
        )

    def own(w):
        return (
            remote(w_ref.at[w], g_ref.at[w, ring.f], osend.at[w], orecv.at[w], ring.mate),
            pltpu.make_async_copy(w_ref.at[w], g_ref.at[w, ring.f], lsem.at[w]),
        )

    def begin(w):
        for way in (0, 1):
            hop(w, way, 0, None).start()
        for copy in own(w):
            copy.start()

    def piece_of(d, way):
        return way if d == h - 1 else None

    begin(0)
    for w in range(count):
        if w + 1 < count:
            begin(w + 1)

        def step(d, carry):
            for way in (0, 1):
                arrival(w, way, d, None).wait_recv()
                hop(w, way, d + 1, None).start()
                share(w, way, d, None).start()
            return carry

        if h - 2 <= 4:
            for d in range(h - 2):
                step(d, 0)
        else:
            lax.fori_loop(0, h - 2, step, 0)
        for d in (h - 2, h - 1):
            for way in (0, 1):
                arrival(w, way, d, piece_of(d, way)).wait_recv()
                if d == h - 2:
                    hop(w, way, h - 1, way).start()
                share(w, way, d, piece_of(d, way)).start()

        def finish(d, carry):
            for way in (0, 1):
                hop(w, way, d, None).wait_send()
                share(w, way, d, None).wait_send()
                share_in(w, way, d, None).wait_recv()
            return carry

        if h - 1 <= 4:
            for d in range(h - 1):
                finish(d, 0)
        else:
            lax.fori_loop(0, h - 1, finish, 0)
        for way in (0, 1):
            hop(w, way, h - 1, way).wait_send()
            share(w, way, h - 1, way).wait_send()
            share_in(w, way, h - 1, way).wait_recv()
        first, second = own(w)
        first.wait_send()
        remote(
            g_ref.at[w, ring.mate[0]],
            g_ref.at[w, ring.mate[0]],
            osend.at[w],
            orecv.at[w],
            ring.mate,
        ).wait_recv()
        second.wait()


def gather_weights(shards, n):
    count, rows, width = shards.shape
    dma = pltpu.SemaphoreType.DMA
    return pl.pallas_call(
        functools.partial(gather_kernel, n),
        out_shape=jax.ShapeDtypeStruct((count, 2 * n, rows, width), shards.dtype),
        in_specs=[pl.BlockSpec(memory_space=pl.ANY)],
        out_specs=pl.BlockSpec(memory_space=pl.ANY),
        scratch_shapes=[
            dma((count, 2, 4)),
            dma((count, 2, 4)),
            dma((count, 2, 4)),
            dma((count, 2, 4)),
            dma((count,)),
            dma((count,)),
            dma((count,)),
        ],
        compiler_params=pltpu.CompilerParams(collective_id=0, has_side_effects=True),
        name="gather_weights",
    )(shards)


def scatter_kernel(
    n,
    left_hbm,
    right_hbm,
    out_hbm,
    left,
    right,
    partial,
    mate_out,
    mate_in,
    ring_in,
    ring_out,
    stage,
    lsem,
    rsem,
    msend,
    mrecv,
    ssem,
    isem,
    osem,
):
    ring = Ring(n)
    h = ring.h
    count = right.shape[0]
    rows = mate_out.shape[1]
    half = rows // 2
    wide = mate_out.shape[2]
    tile = 512
    tiles = wide // tile
    load_left = [pltpu.make_async_copy(left_hbm.at[i], left.at[i], lsem.at[i]) for i in range(4)]
    load_right = [pltpu.make_async_copy(right_hbm.at[i], right.at[i], rsem.at[i]) for i in range(4)]
    for i in range(4):
        load_left[i].start()
        load_right[i].start()
    ring.greet()
    for i in range(4):
        load_left[i].wait()
        load_right[i].wait()

    def mate_copy(pslot, slot):
        return remote(
            mate_out.at[pslot], mate_in.at[slot], msend.at[pslot], mrecv.at[slot], ring.mate
        )

    def prepare(w, dest, sub, pslot, slot):
        base = pl.multiple_of(ring.chip(dest) * (2 * rows), 2 * rows)

        def one(i, carry):
            col = pl.multiple_of(i * tile, tile)
            source = pl.multiple_of(sub * wide + i * tile, tile)
            which = w - w // 2 + (w // 3) * ((sub * tiles + i) // (3 * tiles // 2))
            partial[pslot, :, pl.ds(col, tile)] = jnp.dot(
                left[which, pl.ds(base, 2 * rows), :],
                right[w, :, pl.ds(source, tile)],
                preferred_element_type=jnp.float32,
            )
            mate_out[pslot, :, pl.ds(col, tile)] = partial[
                pslot, pl.ds(pl.multiple_of((1 - ring.c) * rows, rows), rows), pl.ds(col, tile)
            ].astype(jnp.bfloat16)
            return carry

        lax.fori_loop(0, tiles, one, 0)
        mate_copy(pslot, slot).start()

    def ring_copy(way, s, sub, span):
        view = pl.ds(0, rows) if span is None else pl.ds(span * half, half)
        return remote(
            ring_out.at[way, sub, view, :],
            ring_in.at[way, s % 4, sub, view, :],
            ssem.at[way, sub],
            isem.at[way, s % 4, sub],
            ring.next if way == 0 else ring.prev,
        )

    def mine(pslot, slot, col, lo, size):
        start = pl.multiple_of(ring.c * rows + lo, half)
        return partial[pslot, pl.ds(start, size), pl.ds(col, tile)] + mate_in[
            slot, pl.ds(lo, size), pl.ds(col, tile)
        ].astype(jnp.float32)

    def over_tiles(fn):
        def one(i, carry):
            fn(pl.multiple_of(i * tile, tile))
            return carry

        lax.fori_loop(0, tiles, one, 0)

    def arrived(pslot, slot):
        mate_copy(pslot, slot).wait_recv()

    def group(entries, w):
        def lead(k):
            dest, sub, slot, _ = entries[k]
            if k >= 2:
                mate_copy(k % 2, slot).wait_send()
            prepare(w, dest, sub, k % 2, slot)

        lead(0)
        for k, (dest, sub, slot, act) in enumerate(entries):
            if k + 1 < len(entries):
                lead(k + 1)
            arrived(k % 2, slot)
            act(k % 2, slot)
        for k in range(len(entries))[-2:]:
            mate_copy(k % 2, entries[k][2]).wait_send()

    def weight(w, carry):
        def first(sub):
            def act(pslot, slot):
                @pl.when(w > 0)
                def _():
                    for way in (0, 1):
                        ring_copy(way, h - 1, sub, None).wait_send()

                def fill(col):
                    for way in (0, 1):
                        lo = way * half
                        ring_out[way, sub, pl.ds(lo, half), pl.ds(col, tile)] = mine(
                            pslot, slot, col, lo, half
                        ).astype(jnp.bfloat16)

                over_tiles(fill)
                for way in (0, 1):
                    ring_copy(way, 0, sub, way).start()

            return act

        def second(way, sub):
            def act(pslot, slot):
                ring_copy(way, 0, sub, way).wait()

                def fill(col):
                    for part in (0, 1):
                        lo = part * half
                        total = mine(pslot, slot, col, lo, half)
                        if part == way:
                            total = total + ring_in[
                                way, 0, sub, pl.ds(lo, half), pl.ds(col, tile)
                            ].astype(jnp.float32)
                        ring_out[way, sub, pl.ds(lo, half), pl.ds(col, tile)] = total.astype(
                            jnp.bfloat16
                        )

                over_tiles(fill)
                ring_copy(way, 1, sub, None).start()

            return act

        def later(way, sub, s):
            def act(pslot, slot):
                ring_copy(way, s - 1, sub, None).wait()

                def fill(col):
                    total = mine(pslot, slot, col, 0, rows) + ring_in[
                        way, (s - 1) % 4, sub, :, pl.ds(col, tile)
                    ].astype(jnp.float32)
                    ring_out[way, sub, :, pl.ds(col, tile)] = total.astype(jnp.bfloat16)

                over_tiles(fill)
                ring_copy(way, s, sub, None).start()

            return act

        group([(h, sub, sub, first(sub)) for sub in (0, 1)], w)

        @pl.when(w > 0)
        def _():
            last(w - 1)

        group(
            [
                ((h - 1) * (1 - 2 * way), sub, 4 + 2 * way + sub, second(way, sub))
                for way in (0, 1)
                for sub in (0, 1)
            ],
            w,
        )

        def middle(s, carry):
            group(
                [
                    (
                        (h - s) * (1 - 2 * way),
                        sub,
                        4 * (s % 2) + 2 * way + sub,
                        later(way, sub, s),
                    )
                    for way in (0, 1)
                    for sub in (0, 1)
                ],
                w,
            )
            return carry

        lax.fori_loop(2, h, middle, 0)
        return carry

    def result(w, sub):
        return pltpu.make_async_copy(
            stage.at[sub], out_hbm.at[w, :, pl.ds(sub * wide, wide)], osem.at[sub]
        )

    def last(w):
        def final(sub):
            def act(pslot, slot):
                for way in (0, 1):
                    ring_copy(way, h - 1, sub, None).wait_recv()

                @pl.when(w > 0)
                def _():
                    result(w - 1, sub).wait()

                def fill(col):
                    total = mine(pslot, slot, col, 0, rows)
                    for way in (0, 1):
                        total = total + ring_in[
                            way, (h - 1) % 4, sub, :, pl.ds(col, tile)
                        ].astype(jnp.float32)
                    stage[sub, :, pl.ds(col, tile)] = total

                over_tiles(fill)
                result(w, sub).start()

            return act

        group([(0, sub, 2 + sub, final(sub)) for sub in (0, 1)], w)

    lax.fori_loop(0, count, weight, 0)
    last(count - 1)
    for sub in (0, 1):
        for way in (0, 1):
            ring_copy(way, h - 1, sub, None).wait_send()
        result(count - 1, sub).wait()


def scatter_gradients(left, right, n):
    count, length, width = right.shape
    rows = left.shape[1] // (2 * n)
    wide = width // 2
    dma = pltpu.SemaphoreType.DMA
    bf, f32 = jnp.bfloat16, jnp.float32
    return pl.pallas_call(
        functools.partial(scatter_kernel, n),
        out_shape=jax.ShapeDtypeStruct((count, rows, width), f32),
        in_specs=[pl.BlockSpec(memory_space=pl.ANY)] * 2,
        out_specs=pl.BlockSpec(memory_space=pl.ANY),
        scratch_shapes=[
            pltpu.VMEM(left.shape, bf),
            pltpu.VMEM(right.shape, bf),
            pltpu.VMEM((2, 2 * rows, wide), f32),
            pltpu.VMEM((2, rows, wide), bf),
            pltpu.VMEM((8, rows, wide), bf),
            pltpu.VMEM((2, 4, 2, rows, wide), bf),
            pltpu.VMEM((2, 2, rows, wide), bf),
            pltpu.VMEM((2, rows, wide), f32),
            dma((4,)),
            dma((4,)),
            dma((2,)),
            dma((8,)),
            dma((2, 2)),
            dma((2, 4, 2)),
            dma((2,)),
        ],
        compiler_params=pltpu.CompilerParams(
            collective_id=1, has_side_effects=True, vmem_limit_bytes=56 * 1024 * 1024
        ),
        name="scatter_gradients",
    )(left, right)


def both(own):
    return jnp.concatenate([own, lax.ppermute(own, "tensor", SWAP)], axis=0)


def reduce_rows(part):
    rows = part.shape[0] // 2
    other = lax.ppermute(part[rows:].astype(jnp.bfloat16), "tensor", SWAP)
    return part[:rows] + other.astype(jnp.float32)


def doc_positions(segment_row):
    length = segment_row.shape[0]
    indices = jnp.arange(length, dtype=jnp.int32)
    change = jnp.concatenate([jnp.ones((1,), jnp.bool_), segment_row[1:] != segment_row[:-1]])
    begins = lax.cummax(jnp.where(change, indices, 0), axis=0)
    return indices - begins


def rope_tables(positions):
    halfway = HEAD_DIM // 2
    inverse = rope_theta ** (-(jnp.arange(halfway, dtype=jnp.float32) * 2.0) / HEAD_DIM)
    angles = positions.astype(jnp.float32)[:, None] * inverse[None, :]
    return (jnp.cos(angles), jnp.sin(angles))


def rotate(field, cosine, sine_table):
    halfway = field.shape[-1] // 2
    first_half = field[..., :halfway]
    second = field[..., halfway:]
    cos_wide = cosine[:, None, :]
    sin_wide = sine_table[:, None, :]
    return jnp.concatenate(
        [first_half * cos_wide - second * sin_wide, second * cos_wide + first_half * sin_wide],
        axis=-1,
    )


def unrotate(field, cosine, sine_table):
    return rotate(field, cosine, -sine_table)


def norm_back(upstream, normed, factor, gain):
    scaled = upstream * gain
    return factor * (scaled - normed * jnp.mean(scaled * normed, axis=1, keepdims=True))


def attention_scores(queries_r, keys_r, allowed):
    scores = jnp.einsum(
        "qhd,khd->hqk", queries_r, keys_r, preferred_element_type=jnp.float32
    ) * HEAD_DIM ** (-0.5)
    return jnp.where(allowed[None], scores, masked_score)


def product(left, right):
    return jnp.dot(left, right, preferred_element_type=jnp.float32)


def product_t(left, right):
    return lax.dot_general(
        left, right, (((1,), (1,)), ((), ())), preferred_element_type=jnp.float32
    )


def body(
    n,
    tokens,
    segment_ids,
    w_query,
    w_key,
    w_value,
    w_out,
    w_gate,
    w_up,
    w_down,
    gain_query,
    gain_key,
    gain_attn,
    gain_ffn,
    cotangent,
):
    width = w_query.shape[1]
    shards = jnp.stack(
        [
            jnp.concatenate([w_query, w_key, w_value, w_out.T], axis=1),
            w_gate,
            w_up,
            w_down.T,
        ]
    )
    gathered = both(tokens)
    gains = lax.all_gather(
        jnp.stack([gain_query, gain_key, gain_attn, gain_ffn]), "fsdp", axis=1, tiled=True
    ).astype(jnp.float32)
    weights = gather_weights(shards, n)
    D = gains.shape[1]
    weights = weights.reshape(4, D, shards.shape[2])
    query_full = weights[0, :, :width]
    key_full = weights[0, :, width : 2 * width]
    value_full = weights[0, :, 2 * width : 3 * width]
    out_t = weights[0, :, 3 * width :]
    gate_full, up_full, down_t = weights[1], weights[2], weights[3]

    rank = lax.axis_index("tensor")
    heads_here = width // HEAD_DIM
    start_col = rank * width
    gain_query_here = lax.dynamic_slice_in_dim(gains[0], start_col, width)
    gain_key_here = lax.dynamic_slice_in_dim(gains[1], start_col, width)
    attn_gain_f = gains[2]
    ffn_gain_f = gains[3]
    length = gathered.shape[0]
    rows = length // 2
    segment_row = segment_ids[0]

    def arrange(row):
        flat = lax.dynamic_slice_in_dim(jnp.concatenate([row, row]), rank * rows, length)
        return flat

    indices = arrange(jnp.arange(length, dtype=jnp.int32))
    positions = arrange(doc_positions(segment_row))
    segments = arrange(segment_row)
    cosine, sine_table = rope_tables(positions)
    allowed = (segments[:, None] == segments[None, :]) & (indices[:, None] >= indices[None, :])

    queries = product(gathered, query_full)
    key_rows = product(gathered, key_full)
    values = product(gathered, value_full).astype(jnp.bfloat16)
    squares = jnp.stack([jnp.sum(queries * queries, axis=1), jnp.sum(key_rows * key_rows, axis=1)])
    squares = squares + jnp.roll(lax.ppermute(squares, "tensor", SWAP), rows, axis=1)
    query_factor = lax.rsqrt(squares[0] / D + epsilon_norm)[:, None]
    key_factor = lax.rsqrt(squares[1] / D + epsilon_norm)[:, None]
    query_hat = queries * query_factor
    key_hat = key_rows * key_factor
    queries_r = rotate(
        (query_hat * gain_query_here).reshape(length, heads_here, HEAD_DIM), cosine, sine_table
    ).astype(jnp.bfloat16)
    keys_r = rotate(
        (key_hat * gain_key_here).reshape(length, heads_here, HEAD_DIM), cosine, sine_table
    ).astype(jnp.bfloat16)
    values_r = values.reshape(length, heads_here, HEAD_DIM)
    scores = attention_scores(queries_r, keys_r, allowed)
    top_score = jnp.max(scores, axis=-1, keepdims=True)
    log_total = top_score + jnp.log(jnp.sum(jnp.exp(scores - top_score), axis=-1, keepdims=True))
    attn_probs = jnp.exp(scores - log_total).astype(jnp.bfloat16)
    attended = (
        jnp.einsum("hqk,khd->qhd", attn_probs, values_r, preferred_element_type=jnp.float32)
        .astype(jnp.bfloat16)
        .reshape(length, width)
    )
    attn_rows = reduce_rows(product_t(attended, out_t))
    attn_factor = lax.rsqrt(jnp.mean(attn_rows * attn_rows, axis=1) + epsilon_norm)[:, None]
    attn_hat = attn_rows * attn_factor
    middle = tokens.astype(jnp.float32) + attn_hat * attn_gain_f
    middle_all = both(middle.astype(jnp.bfloat16))
    gate_pre = product(middle_all, gate_full)
    up_proj = product(middle_all, up_full)
    sigmoid_gate = jax.nn.sigmoid(gate_pre)
    silu_gate = gate_pre * sigmoid_gate
    hidden = (silu_gate * up_proj).astype(jnp.bfloat16)
    down_rows = reduce_rows(product_t(hidden, down_t))
    down_factor = lax.rsqrt(jnp.mean(down_rows * down_rows, axis=1) + epsilon_norm)[:, None]
    down_hat = down_rows * down_factor
    layer_out = (middle + down_hat * ffn_gain_f).astype(jnp.bfloat16)

    grad_out = cotangent.astype(jnp.float32)
    ffn_gain_grad = jnp.sum(grad_out * down_hat, axis=0)
    grad_down = norm_back(grad_out, down_hat, down_factor, ffn_gain_f).astype(jnp.bfloat16)
    grad_down_all = both(grad_down)
    grad_hidden = product(grad_down_all, down_t)
    grad_gate = (
        grad_hidden * up_proj * sigmoid_gate * (1.0 + gate_pre * (1.0 - sigmoid_gate))
    ).astype(jnp.bfloat16)
    grad_up = (grad_hidden * silu_gate).astype(jnp.bfloat16)
    grad_middle = grad_out + reduce_rows(
        product_t(grad_gate, gate_full) + product_t(grad_up, up_full)
    )
    attn_gain_grad = jnp.sum(grad_middle * attn_hat, axis=0)
    grad_attn = norm_back(grad_middle, attn_hat, attn_factor, attn_gain_f).astype(jnp.bfloat16)
    grad_attn_all = both(grad_attn)
    grad_attended = (
        product(grad_attn_all, out_t).astype(jnp.bfloat16).reshape(length, heads_here, HEAD_DIM)
    )
    probs_again = jnp.exp(attention_scores(queries_r, keys_r, allowed) - log_total)
    grad_values = jnp.einsum(
        "hqk,qhd->khd",
        probs_again.astype(jnp.bfloat16),
        grad_attended,
        preferred_element_type=jnp.float32,
    ).astype(jnp.bfloat16)
    grad_probs = jnp.einsum(
        "qhd,khd->hqk", grad_attended, values_r, preferred_element_type=jnp.float32
    )
    grad_scores = (
        probs_again * (grad_probs - jnp.sum(probs_again * grad_probs, axis=-1, keepdims=True))
    ).astype(jnp.bfloat16)
    score_scale = HEAD_DIM ** (-0.5)
    grad_queries_r = (
        jnp.einsum("hqk,khd->qhd", grad_scores, keys_r, preferred_element_type=jnp.float32)
        * score_scale
    )
    grad_keys_r = (
        jnp.einsum("hqk,qhd->khd", grad_scores, queries_r, preferred_element_type=jnp.float32)
        * score_scale
    )
    grad_query_n = unrotate(grad_queries_r, cosine, sine_table).reshape(length, width)
    grad_key_n = unrotate(grad_keys_r, cosine, sine_table).reshape(length, width)
    query_gain_part = jnp.sum(grad_query_n * query_hat, axis=0)
    key_gain_part = jnp.sum(grad_key_n * key_hat, axis=0)
    query_scaled = grad_query_n * gain_query_here
    key_scaled = grad_key_n * gain_key_here
    dots = jnp.stack(
        [jnp.sum(query_scaled * query_hat, axis=1), jnp.sum(key_scaled * key_hat, axis=1)]
    )
    dots = dots + jnp.roll(lax.ppermute(dots, "tensor", SWAP), rows, axis=1)
    grad_queries = (query_factor * (query_scaled - query_hat * (dots[0] / D)[:, None])).astype(
        jnp.bfloat16
    )
    grad_keys = (key_factor * (key_scaled - key_hat * (dots[1] / D)[:, None])).astype(jnp.bfloat16)
    grad_values_flat = grad_values.reshape(length, width)
    grads_qkv = jnp.concatenate([grad_queries, grad_keys, grad_values_flat], axis=1)
    grad_input = grad_middle + reduce_rows(product_t(grads_qkv, weights[0, :, : 3 * width]))

    zeros = jnp.zeros((D,), jnp.float32)
    gain_parts = jnp.stack(
        [
            lax.dynamic_update_slice_in_dim(zeros, query_gain_part, start_col, 0),
            lax.dynamic_update_slice_in_dim(zeros, key_gain_part, start_col, 0),
            attn_gain_grad,
            ffn_gain_grad,
        ]
    )
    gain_sums = lax.psum(gain_parts, ("fsdp", "tensor"))
    share = D // (2 * n)
    gain_grads = lax.dynamic_slice_in_dim(gain_sums, lax.axis_index("fsdp") * share, share, axis=1)

    left = jnp.stack([grad_down_all.T, middle_all.T, gathered.T, grad_attn_all.T])
    right = jnp.stack(
        [hidden, grad_up, grad_gate, jnp.concatenate([grads_qkv, attended], axis=1)]
    )
    grads = scatter_gradients(left, right, n)
    first = grads[3]
    return (
        layer_out,
        grad_input,
        first[:, :width],
        first[:, width : 2 * width],
        first[:, 2 * width : 3 * width],
        first[:, 3 * width :].T,
        grads[2],
        grads[1],
        grads[0].T,
        gain_grads[0],
        gain_grads[1],
        gain_grads[2],
        gain_grads[3],
    )


def solution(mesh):
    rows, cols, gain = P("fsdp", "tensor"), P("tensor", "fsdp"), P("fsdp")
    acts = P(("fsdp", "tensor"), None)
    return jax.shard_map(
        functools.partial(body, mesh.shape["fsdp"] // 2),
        mesh=mesh,
        in_specs=(acts, P("fsdp", None), rows, rows, rows, cols, rows, rows, cols)
        + (gain,) * 4
        + (acts,),
        out_specs=(acts, acts, rows, rows, rows, cols, rows, rows, cols) + (gain,) * 4,
        check_vma=False,
    )
```

```python
import functools

import jax
import jax.numpy as jnp
from jax import lax
from jax.experimental import pallas as pl
from jax.experimental.pallas import tpu as pltpu
from jax.sharding import PartitionSpec as P

HEAD_DIM = 128
epsilon_norm = 1e-06
rope_theta = 500000.0
masked_score = -1e30
MESH = pl.DeviceIdType.MESH
SWAP = [(0, 1), (1, 0)]


def ring_chip(pos, n):
    if n != 8:
        return pos
    x = pos // 4
    z = pos + x * (7 - 2 * pos)
    return z * 2 + x


def ring_pos(chip, n):
    if n != 8:
        return chip
    x = chip % 2
    z = chip // 2
    return z + x * (7 - 2 * z)


class Ring:
    def __init__(self, n):
        self.n = n
        self.h = n // 2
        self.f = lax.axis_index("fsdp")
        self.t = lax.axis_index("tensor")
        self.c = self.f % 2
        self.pos = ring_pos(self.f // 2, n)
        self.next = (self.chip(1) * 2 + self.c, self.t)
        self.prev = (self.chip(-1) * 2 + self.c, self.t)
        self.mate = (self.f + 1 - 2 * self.c, self.t)
        self.partner = (self.f, 1 - self.t)

    def chip(self, offset):
        return ring_chip((self.pos + offset + self.n) % self.n, self.n)

    def greet(self):
        barrier = pltpu.get_barrier_semaphore()
        for peer in (self.next, self.prev, self.mate, self.partner):
            pl.semaphore_signal(barrier, inc=1, device_id=peer, device_id_type=MESH)
        pl.semaphore_wait(barrier, 4)


def remote(src, dst, send, recv, peer):
    return pltpu.make_async_remote_copy(
        src_ref=src,
        dst_ref=dst,
        send_sem=send,
        recv_sem=recv,
        device_id=peer,
        device_id_type=MESH,
    )


def repeat(lo, hi, fn):
    if hi - lo <= 4:
        for i in range(lo, hi):
            fn(i)
    else:

        def one(i, carry):
            fn(i)
            return carry

        lax.fori_loop(lo, hi, one, 0)


def loop(count, fn):
    def one(i, carry):
        fn(i)
        return carry

    lax.fori_loop(0, count, one, 0)


def nt_dot(left, right):
    return lax.dot_general(
        left, right, (((1,), (1,)), ((), ())), preferred_element_type=jnp.float32
    )


def nn_dot(left, right):
    return jnp.dot(left, right, preferred_element_type=jnp.float32)


class Stream:
    def __init__(self, g_ref, wcol, wrow, sem):
        self.g, self.wcol, self.wrow, self.sem = g_ref, wcol, wrow, sem

    def cols(self, w, start, count, fn):
        tile = self.wcol.shape[2]

        def copy(j):
            col = pl.multiple_of(start + j * tile, tile)
            return pltpu.make_async_copy(
                self.g.at[w, :, pl.ds(col, tile)], self.wcol.at[j % 2], self.sem.at[j % 2]
            )

        copy(0).start()

        def one(j):
            @pl.when(j + 1 < count)
            def _():
                copy(j + 1).start()

            copy(j).wait()
            fn(j, self.wcol.at[j % 2])

        loop(count, one)

    def row_copy(self, w, chunk, slot, start, width):
        size = self.wrow.shape[1]
        return pltpu.make_async_copy(
            self.g.at[w, pl.ds(pl.multiple_of(chunk * size, size), size), pl.ds(start, width)],
            self.wrow.at[slot, :, pl.ds(0, width)],
            self.sem.at[slot],
        )

    def rows(self, w, start, width, fn):
        count = self.g.shape[1] // self.wrow.shape[1]
        self.row_copy(w, 0, 0, start, width).start()

        def one(j):
            @pl.when(j + 1 < count)
            def _():
                self.row_copy(w, j + 1, (j + 1) % 2, start, width).start()

            self.row_copy(w, j, j % 2, start, width).wait()
            fn(j, self.wrow.at[j % 2, :, pl.ds(0, width)])

        loop(count, one)


def forward_kernel(
    n,
    w_ref,
    tok_ref,
    cot_ref,
    gain_ref,
    cos_ref,
    sin_ref,
    bias_ref,
    g_ref,
    out_ref,
    x_out,
    hat_out,
    qr_out,
    kr_out,
    v_out,
    o_out,
    ahat_out,
    mb_out,
    silu_out,
    slope_out,
    hid_out,
    df_out,
    fac_ref,
    gffn_ref,
    x,
    cot,
    hat,
    qr,
    kr,
    v,
    o,
    sq,
    sq_in,
    part,
    part_out,
    part_in,
    down_in,
    ahat,
    mid,
    mb,
    gate,
    up,
    silu,
    slope,
    hid,
    df,
    wcol,
    wrow,
    ssem,
    rsem,
    msend,
    mrecv,
    osend,
    orecv,
    lsem,
    wsem,
    ysend,
    yrecv,
    fsend,
    frecv,
    save_sem,
):
    ring = Ring(n)
    h = ring.h
    count, rows, _ = w_ref.shape
    piece_half = rows // 2
    own_rows = tok_ref.shape[0]
    length = 2 * own_rows
    D = x.shape[1]
    local = v.shape[1]
    heads = local // HEAD_DIM
    chunk = wrow.shape[1]

    load = [
        pltpu.make_async_copy(tok_ref, x.at[pl.ds(0, own_rows), :], lsem.at[count]),
        pltpu.make_async_copy(cot_ref, cot.at[pl.ds(0, own_rows), :], lsem.at[count + 1]),
    ]
    for copy in load:
        copy.start()
    ring.greet()

    def spot(w, s):
        return g_ref.at[w, pl.ds(pl.multiple_of(s * rows, rows), rows), :]

    def cut(ref, piece):
        if piece is None:
            return ref
        return ref.at[pl.ds(piece * piece_half, piece_half), :]

    def piece_of(d, way):
        return way if isinstance(d, int) and d == h - 1 else None

    def away(way, d):
        return ring.chip(-d if way == 0 else d) * 2

    def hop(w, way, d):
        piece = piece_of(d, way)
        s = away(way, d) + ring.c
        src = w_ref.at[w] if isinstance(d, int) and d == 0 else spot(w, s)
        return remote(
            cut(src, piece),
            cut(spot(w, s), piece),
            ssem.at[w, way, d % 4],
            rsem.at[w, way, d % 4],
            ring.next if way == 0 else ring.prev,
        )

    def arrival(w, way, d):
        ref = cut(spot(w, away(way, d + 1) + ring.c), piece_of(d, way))
        return remote(
            ref,
            ref,
            ssem.at[w, way, d % 4],
            rsem.at[w, way, d % 4],
            ring.next if way == 0 else ring.prev,
        )

    def share(w, way, d, core):
        ref = cut(spot(w, away(way, d + 1) + core), piece_of(d, way))
        return remote(ref, ref, msend.at[w, way, d % 4], mrecv.at[w, way, d % 4], ring.mate)

    def own_mate(w):
        return remote(w_ref.at[w], spot(w, ring.f), osend.at[w], orecv.at[w], ring.mate)

    def own_here(w):
        return pltpu.make_async_copy(w_ref.at[w], spot(w, ring.f), lsem.at[w])

    def begin(w):
        for way in (0, 1):
            hop(w, way, 0).start()
        own_mate(w).start()
        own_here(w).start()

    def step(w, d):
        for way in (0, 1):
            arrival(w, way, d).wait_recv()
            if not isinstance(d, int) or d < h - 1:
                hop(w, way, d + 1).start()
            share(w, way, d, ring.c).start()

    def steps(w, lo, hi):
        first, last = lo * h // 4, hi * h // 4
        repeat(first, min(last, h - 2), lambda d: step(w, d))
        for d in range(max(first, h - 2), last):
            step(w, d)

    def shared(w, lo, hi):
        def one(d):
            for way in (0, 1):
                share(w, way, d, 1 - ring.c).wait_recv()

        repeat(lo, min(hi, h - 1), one)
        if hi == h:
            one(h - 1)

    def own_shared(w):
        ref = spot(w, ring.mate[0])
        remote(ref, ref, osend.at[w], orecv.at[w], ring.mate).wait_recv()
        own_here(w).wait()

    def complete(w):
        own_shared(w)
        shared(w, 0, h)

    partner = (ring.f, 1 - ring.t)

    def swap(i, src, dst):
        return remote(src, dst, ysend.at[i], yrecv.at[i], partner)

    low, high = pl.ds(0, own_rows), pl.ds(own_rows, own_rows)
    swaps = [
        swap(0, tok_ref, x.at[high, :]),
        swap(1, cot_ref, cot.at[high, :]),
        swap(2, sq.at[low, :], sq_in.at[high, :]),
        swap(3, sq.at[high, :], sq_in.at[low, :]),
        swap(4, part_out, part_in),
    ]

    def sum_copy(k, width):
        view = pl.ds(pl.multiple_of(k * width, width), width)
        return remote(
            part_out.at[:, view], down_in.at[:, view], fsend.at[k], frecv.at[k], partner
        )

    saves = []

    def save(src, dst):
        copy = pltpu.make_async_copy(src, dst, save_sem.at[len(saves)])
        copy.start()
        saves.append(copy)

    stream = Stream(g_ref, wcol, wrow, wsem)

    begin(0)
    swaps[0].start()
    swaps[1].start()
    steps(0, 0, 1)
    begin(1)
    steps(0, 1, 4)
    load[0].wait()
    swaps[0].wait_recv()
    save(x, x_out)
    complete(0)

    tile = wcol.shape[2]
    lane = lax.broadcasted_iota(jnp.int32, (length, HEAD_DIM), 1)
    sq[...] = jnp.zeros_like(sq)

    def query_key(j, w):
        acc = nn_dot(x[...], w[...])
        hat[:, pl.ds(pl.multiple_of(j * tile, tile), tile)] = acc
        side = (j * tile) // local
        total = jnp.sum(acc * acc, axis=1, keepdims=True)
        sq[...] += jnp.where(lane // (HEAD_DIM // 2) == side, total, 0.0)

    def value(j, w):
        v[:, pl.ds(pl.multiple_of(j * tile, tile), tile)] = nn_dot(x[...], w[...]).astype(
            jnp.bfloat16
        )

    stream.cols(0, 0, 2 * local // tile, query_key)
    swaps[2].start()
    swaps[3].start()
    stream.cols(0, 2 * local, local // tile, value)
    save(v, v_out)
    steps(1, 0, 1)
    begin(2)
    for i in (2, 3):
        swaps[i].wait_recv()
    both_sq = sq[...] + sq_in[...]
    for i in (2, 3):
        swaps[i].wait_send()
    for side in (0, 1):
        col = both_sq[:, side * (HEAD_DIM // 2) : side * (HEAD_DIM // 2) + 1]
        fac_ref[side] = jnp.broadcast_to(
            lax.rsqrt(col / D + epsilon_norm), (length, HEAD_DIM)
        )

    def head(i):
        at = pl.ds(pl.multiple_of(i * HEAD_DIM, HEAD_DIM), HEAD_DIM)
        gain_at = pl.ds(pl.multiple_of(ring.t * local + i * HEAD_DIM, HEAD_DIM), HEAD_DIM)
        for side, dst in ((0, qr), (1, kr)):
            where = pl.ds(pl.multiple_of(side * local + i * HEAD_DIM, HEAD_DIM), HEAD_DIM)
            normed = hat[:, where] * fac_ref[side]
            hat[:, where] = normed
            scaled = normed * gain_ref[side : side + 1, gain_at]
            turned = scaled * cos_ref[...] + pltpu.roll(scaled, HEAD_DIM // 2, 1) * sin_ref[...]
            dst[:, at] = turned.astype(jnp.bfloat16)
        scores = nt_dot(qr[:, at], kr[:, at]) * HEAD_DIM ** (-0.5) + bias_ref[...]
        top = jnp.max(scores, axis=1, keepdims=True)
        raised = jnp.exp(scores - top)
        probs = raised / jnp.sum(raised, axis=1, keepdims=True)
        o[:, at] = nn_dot(probs.astype(jnp.bfloat16), v[:, at]).astype(jnp.bfloat16)

    loop(heads, head)
    save(hat, hat_out)
    save(qr, qr_out)
    save(kr, kr_out)
    save(o, o_out)
    steps(1, 1, 2)

    def split(k, width, acc):
        view = pl.ds(pl.multiple_of(k * width, width), width)
        part[:, view] = acc
        part_out[low, view] = acc[own_rows:].astype(jnp.bfloat16)
        part_out[high, view] = acc[:own_rows].astype(jnp.bfloat16)

    stream.rows(0, 3 * local, local, lambda k, w: split(k, chunk, nt_dot(o[...], w[...])))
    swaps[4].start()
    steps(1, 2, 3)
    swaps[4].wait_recv()

    block = 16

    def norm_rows(i, arrived):
        at = pl.ds(pl.multiple_of(i * block, block), block)
        total = part[at, :] + arrived[at, :].astype(jnp.float32)
        factor = lax.rsqrt(jnp.mean(total * total, axis=1, keepdims=True) + epsilon_norm)
        return at, factor, total * factor

    def attn_norm(i):
        at, factor, normed = norm_rows(i, part_in)
        ahat[at, :] = normed
        fac_ref[2, at, :] = jnp.broadcast_to(factor, (block, HEAD_DIM))
        middle = x[at, :].astype(jnp.float32) + normed * gain_ref[2:3, :]
        mid[at, :] = middle
        mb[at, :] = middle.astype(jnp.bfloat16)

    loop(length // block, attn_norm)
    swaps[4].wait_send()
    save(ahat, ahat_out)
    save(mb, mb_out)
    steps(1, 3, 4)
    complete(1)

    def gate_tile(j, w):
        gate[:, pl.ds(pl.multiple_of(j * tile, tile), tile)] = nn_dot(mb[...], w[...])

    width = gate.shape[1]
    stream.cols(1, 0, width // tile, gate_tile)
    steps(2, 0, 1)
    begin(3)
    steps(2, 1, 4)
    complete(2)

    tall = 64

    def up_tile(j, w):
        up[...] = nn_dot(mb[...], w[...])
        view = pl.ds(pl.multiple_of(j * tile, tile), tile)

        def some(i):
            at = pl.ds(pl.multiple_of(i * tall, tall), tall)
            g = gate[at, view]
            u = up[at, :]
            sig = 1.0 / (1.0 + jnp.exp(-g))
            act = g * sig
            silu[at, view] = act.astype(jnp.bfloat16)
            hid[at, view] = (act * u).astype(jnp.bfloat16)
            slope[at, view] = (u * sig * (1.0 + g * (1.0 - sig))).astype(jnp.bfloat16)

        loop(length // tall, some)

    stream.cols(2, 0, width // tile, up_tile)
    save(silu, silu_out)
    save(slope, slope_out)
    save(hid, hid_out)

    turn = [0]

    def down(k, slot):
        stream.row_copy(3, k, slot, 0, width).wait()
        split(k, chunk, nt_dot(hid[...], wrow[slot]))
        sum_copy(k, chunk).start()

    def fetch(k):
        slot = turn[0] % 2
        turn[0] += 1
        stream.row_copy(3, k, slot, 0, width).start()
        return slot

    chunks = D // chunk
    if chunks == n:
        own_shared(3)
        queue = [(ring.chip(0), fetch(ring.chip(0)))]

        def drain():
            while queue:
                down(*queue.pop(0))

        for d in range(h):
            step(3, d)
            drain()
            shared(3, d, d + 1)
            for way in (0, 1):
                if d < h - 1 or way == 0:
                    k = ring.chip(-1 - d if way == 0 else 1 + d)
                    queue.append((k, fetch(k)))
        drain()
    else:
        steps(3, 0, 4)
        complete(3)
        for k in range(chunks):
            down(k, fetch(k))

    def sums(i):
        sum_copy(i, chunk).wait()

    loop(chunks, sums)
    load[1].wait()
    swaps[1].wait_recv()
    gffn_ref[...] = jnp.zeros_like(gffn_ref)
    gain = gain_ref[3:4, :]

    def ffn_norm(i):
        at, factor, normed = norm_rows(i, down_in)
        y = cot[at, :].astype(jnp.float32)

        @pl.when(i < own_rows // block)
        def _():
            out_ref[at, :] = (mid[at, :] + normed * gain).astype(jnp.bfloat16)
            gffn_ref[0:1, :] += jnp.sum(y * normed, axis=0, keepdims=True)

        scaled = y * gain
        df[at, :] = (
            factor * (scaled - normed * jnp.mean(scaled * normed, axis=1, keepdims=True))
        ).astype(jnp.bfloat16)

    loop(length // block, ffn_norm)
    save(df, df_out)

    for i in (0, 1):
        swaps[i].wait_send()
    for w in range(count):
        def sent(d):
            for way in (0, 1):
                hop(w, way, d).wait_send()
                share(w, way, d, ring.c).wait_send()

        repeat(0, h - 1, sent)
        sent(h - 1)
        own_mate(w).wait_send()
    for copy in saves:
        copy.wait()


def forward(shards, tokens, cotangent, gains, cosine, sine, bias, n):
    count, rows, width = shards.shape
    own_rows, D = tokens.shape
    length = 2 * own_rows
    local = width // 4
    bf, f32 = jnp.bfloat16, jnp.float32
    dma = pltpu.SemaphoreType.DMA
    vm = pltpu.VMEM
    anywhere = pl.BlockSpec(memory_space=pl.ANY)
    inside = pl.BlockSpec(memory_space=pltpu.VMEM)
    struct = jax.ShapeDtypeStruct
    chunk = 256
    saved = [
        struct((length, D), bf),
        struct((length, 2 * local), f32),
        struct((length, local), bf),
        struct((length, local), bf),
        struct((length, local), bf),
        struct((length, local), bf),
        struct((length, D), f32),
        struct((length, D), bf),
        struct((length, width), bf),
        struct((length, width), bf),
        struct((length, width), bf),
        struct((length, D), bf),
    ]
    return pl.pallas_call(
        functools.partial(forward_kernel, n),
        out_shape=[struct((count, D, width), bf), struct((own_rows, D), bf)]
        + saved
        + [struct((3, length, HEAD_DIM), f32), struct((8, D), f32)],
        in_specs=[anywhere] * 3 + [inside] * 4,
        out_specs=[anywhere, inside] + [anywhere] * 12 + [inside] * 2,
        scratch_shapes=[
            vm((length, D), bf),
            vm((length, D), bf),
            vm((length, 2 * local), f32),
            vm((length, local), bf),
            vm((length, local), bf),
            vm((length, local), bf),
            vm((length, local), bf),
            vm((length, HEAD_DIM), f32),
            vm((length, HEAD_DIM), f32),
            vm((length, D), f32),
            vm((length, D), bf),
            vm((length, D), bf),
            vm((length, D), bf),
            vm((length, D), f32),
            vm((length, D), f32),
            vm((length, D), bf),
            vm((length, width), f32),
            vm((length, 512), f32),
            vm((length, width), bf),
            vm((length, width), bf),
            vm((length, width), bf),
            vm((length, D), bf),
            vm((2, D, 512), bf),
            vm((2, chunk, width), bf),
            dma((count, 2, 4)),
            dma((count, 2, 4)),
            dma((count, 2, 4)),
            dma((count, 2, 4)),
            dma((count,)),
            dma((count,)),
            dma((count + 2,)),
            dma((2,)),
            dma((5,)),
            dma((5,)),
            dma((D // chunk,)),
            dma((D // chunk,)),
            dma((12,)),
        ],
        compiler_params=pltpu.CompilerParams(
            collective_id=0, has_side_effects=True, vmem_limit_bytes=60 * 1024 * 1024
        ),
        name="forward",
    )(shards, tokens, cotangent, gains, cosine, sine, bias)


def scatter_kernel(
    n,
    left_hbm,
    right_hbm,
    out_hbm,
    left,
    right,
    partial,
    mate_out,
    mate_in,
    ring_in,
    ring_out,
    stage,
    lsem,
    rsem,
    msend,
    mrecv,
    ssem,
    isem,
    osem,
):
    ring = Ring(n)
    h = ring.h
    count = right.shape[0]
    rows = mate_out.shape[1]
    half = rows // 2
    wide = mate_out.shape[2]
    tile = 512
    tiles = wide // tile
    load_left = [pltpu.make_async_copy(left_hbm.at[i], left.at[i], lsem.at[i]) for i in range(4)]
    load_right = [pltpu.make_async_copy(right_hbm.at[i], right.at[i], rsem.at[i]) for i in range(4)]
    for i in range(4):
        load_left[i].start()
        load_right[i].start()
    ring.greet()
    for i in range(4):
        load_left[i].wait()
        load_right[i].wait()

    def mate_copy(pslot, slot):
        return remote(
            mate_out.at[pslot], mate_in.at[slot], msend.at[pslot], mrecv.at[slot], ring.mate
        )

    def prepare(w, dest, sub, pslot, slot):
        base = pl.multiple_of(ring.chip(dest) * (2 * rows), 2 * rows)

        def one(i, carry):
            col = pl.multiple_of(i * tile, tile)
            source = pl.multiple_of(sub * wide + i * tile, tile)
            which = w - w // 2 + (w // 3) * ((sub * tiles + i) // (3 * tiles // 2))
            partial[pslot, :, pl.ds(col, tile)] = jnp.dot(
                left[which, pl.ds(base, 2 * rows), :],
                right[w, :, pl.ds(source, tile)],
                preferred_element_type=jnp.float32,
            )
            mate_out[pslot, :, pl.ds(col, tile)] = partial[
                pslot, pl.ds(pl.multiple_of((1 - ring.c) * rows, rows), rows), pl.ds(col, tile)
            ].astype(jnp.bfloat16)
            return carry

        lax.fori_loop(0, tiles, one, 0)
        mate_copy(pslot, slot).start()

    def ring_copy(way, s, sub, span):
        view = pl.ds(0, rows) if span is None else pl.ds(span * half, half)
        return remote(
            ring_out.at[way, sub, view, :],
            ring_in.at[way, s % 4, sub, view, :],
            ssem.at[way, sub],
            isem.at[way, s % 4, sub],
            ring.next if way == 0 else ring.prev,
        )

    def mine(pslot, slot, col, lo, size):
        start = pl.multiple_of(ring.c * rows + lo, half)
        return partial[pslot, pl.ds(start, size), pl.ds(col, tile)] + mate_in[
            slot, pl.ds(lo, size), pl.ds(col, tile)
        ].astype(jnp.float32)

    def over_tiles(fn):
        def one(i, carry):
            fn(pl.multiple_of(i * tile, tile))
            return carry

        lax.fori_loop(0, tiles, one, 0)

    def arrived(pslot, slot):
        mate_copy(pslot, slot).wait_recv()

    def group(entries, w):
        def lead(k):
            dest, sub, slot, _ = entries[k]
            if k >= 2:
                mate_copy(k % 2, slot).wait_send()
            prepare(w, dest, sub, k % 2, slot)

        lead(0)
        for k, (dest, sub, slot, act) in enumerate(entries):
            if k + 1 < len(entries):
                lead(k + 1)
            arrived(k % 2, slot)
            act(k % 2, slot)
        for k in range(len(entries))[-2:]:
            mate_copy(k % 2, entries[k][2]).wait_send()

    def weight(w, carry):
        def first(sub):
            def act(pslot, slot):
                @pl.when(w > 0)
                def _():
                    for way in (0, 1):
                        ring_copy(way, h - 1, sub, None).wait_send()

                def fill(col):
                    for way in (0, 1):
                        lo = way * half
                        ring_out[way, sub, pl.ds(lo, half), pl.ds(col, tile)] = mine(
                            pslot, slot, col, lo, half
                        ).astype(jnp.bfloat16)

                over_tiles(fill)
                for way in (0, 1):
                    ring_copy(way, 0, sub, way).start()

            return act

        def second(way, sub):
            def act(pslot, slot):
                ring_copy(way, 0, sub, way).wait()

                def fill(col):
                    for part in (0, 1):
                        lo = part * half
                        total = mine(pslot, slot, col, lo, half)
                        if part == way:
                            total = total + ring_in[
                                way, 0, sub, pl.ds(lo, half), pl.ds(col, tile)
                            ].astype(jnp.float32)
                        ring_out[way, sub, pl.ds(lo, half), pl.ds(col, tile)] = total.astype(
                            jnp.bfloat16
                        )

                over_tiles(fill)
                ring_copy(way, 1, sub, None).start()

            return act

        def later(way, sub, s):
            def act(pslot, slot):
                ring_copy(way, s - 1, sub, None).wait()

                def fill(col):
                    total = mine(pslot, slot, col, 0, rows) + ring_in[
                        way, (s - 1) % 4, sub, :, pl.ds(col, tile)
                    ].astype(jnp.float32)
                    ring_out[way, sub, :, pl.ds(col, tile)] = total.astype(jnp.bfloat16)

                over_tiles(fill)
                ring_copy(way, s, sub, None).start()

            return act

        group([(h, sub, sub, first(sub)) for sub in (0, 1)], w)

        @pl.when(w > 0)
        def _():
            last(w - 1)

        group(
            [
                ((h - 1) * (1 - 2 * way), sub, 4 + 2 * way + sub, second(way, sub))
                for way in (0, 1)
                for sub in (0, 1)
            ],
            w,
        )

        def middle(s, carry):
            group(
                [
                    (
                        (h - s) * (1 - 2 * way),
                        sub,
                        4 * (s % 2) + 2 * way + sub,
                        later(way, sub, s),
                    )
                    for way in (0, 1)
                    for sub in (0, 1)
                ],
                w,
            )
            return carry

        lax.fori_loop(2, h, middle, 0)
        return carry

    def result(w, sub):
        return pltpu.make_async_copy(
            stage.at[sub], out_hbm.at[w, :, pl.ds(sub * wide, wide)], osem.at[sub]
        )

    def last(w):
        def final(sub):
            def act(pslot, slot):
                for way in (0, 1):
                    ring_copy(way, h - 1, sub, None).wait_recv()

                @pl.when(w > 0)
                def _():
                    result(w - 1, sub).wait()

                def fill(col):
                    total = mine(pslot, slot, col, 0, rows)
                    for way in (0, 1):
                        total = total + ring_in[
                            way, (h - 1) % 4, sub, :, pl.ds(col, tile)
                        ].astype(jnp.float32)
                    stage[sub, :, pl.ds(col, tile)] = total

                over_tiles(fill)
                result(w, sub).start()

            return act

        group([(0, sub, 2 + sub, final(sub)) for sub in (0, 1)], w)

    lax.fori_loop(0, count, weight, 0)
    last(count - 1)
    for sub in (0, 1):
        for way in (0, 1):
            ring_copy(way, h - 1, sub, None).wait_send()
        result(count - 1, sub).wait()


def scatter_gradients(left, right, n):
    count, length, width = right.shape
    rows = left.shape[1] // (2 * n)
    wide = width // 2
    dma = pltpu.SemaphoreType.DMA
    bf, f32 = jnp.bfloat16, jnp.float32
    return pl.pallas_call(
        functools.partial(scatter_kernel, n),
        out_shape=jax.ShapeDtypeStruct((count, rows, width), f32),
        in_specs=[pl.BlockSpec(memory_space=pl.ANY)] * 2,
        out_specs=pl.BlockSpec(memory_space=pl.ANY),
        scratch_shapes=[
            pltpu.VMEM(left.shape, bf),
            pltpu.VMEM(right.shape, bf),
            pltpu.VMEM((2, 2 * rows, wide), f32),
            pltpu.VMEM((2, rows, wide), bf),
            pltpu.VMEM((8, rows, wide), bf),
            pltpu.VMEM((2, 4, 2, rows, wide), bf),
            pltpu.VMEM((2, 2, rows, wide), bf),
            pltpu.VMEM((2, rows, wide), f32),
            dma((4,)),
            dma((4,)),
            dma((2,)),
            dma((8,)),
            dma((2, 2)),
            dma((2, 4, 2)),
            dma((2,)),
        ],
        compiler_params=pltpu.CompilerParams(
            collective_id=1, has_side_effects=True, vmem_limit_bytes=56 * 1024 * 1024
        ),
        name="scatter_gradients",
    )(left, right)


def both(own):
    return jnp.concatenate([own, lax.ppermute(own, "tensor", SWAP)], axis=0)


def reduce_rows(part):
    rows = part.shape[0] // 2
    other = lax.ppermute(part[rows:].astype(jnp.bfloat16), "tensor", SWAP)
    return part[:rows] + other.astype(jnp.float32)


def doc_positions(segment_row):
    length = segment_row.shape[0]
    indices = jnp.arange(length, dtype=jnp.int32)
    change = jnp.concatenate([jnp.ones((1,), jnp.bool_), segment_row[1:] != segment_row[:-1]])
    begins = lax.cummax(jnp.where(change, indices, 0), axis=0)
    return indices - begins


def rope_tables(positions):
    halfway = HEAD_DIM // 2
    inverse = rope_theta ** (-(jnp.arange(halfway, dtype=jnp.float32) * 2.0) / HEAD_DIM)
    angles = positions.astype(jnp.float32)[:, None] * inverse[None, :]
    return (jnp.cos(angles), jnp.sin(angles))


def rotate(field, cosine, sine_table):
    halfway = field.shape[-1] // 2
    first_half = field[..., :halfway]
    second = field[..., halfway:]
    cos_wide = cosine[:, None, :]
    sin_wide = sine_table[:, None, :]
    return jnp.concatenate(
        [first_half * cos_wide - second * sin_wide, second * cos_wide + first_half * sin_wide],
        axis=-1,
    )


def unrotate(field, cosine, sine_table):
    return rotate(field, cosine, -sine_table)


def norm_back(upstream, normed, factor, gain):
    scaled = upstream * gain
    return factor * (scaled - normed * jnp.mean(scaled * normed, axis=1, keepdims=True))


def attention_scores(queries_r, keys_r, allowed):
    scores = jnp.einsum(
        "qhd,khd->hqk", queries_r, keys_r, preferred_element_type=jnp.float32
    ) * HEAD_DIM ** (-0.5)
    return jnp.where(allowed[None], scores, masked_score)


def product(left, right):
    return jnp.dot(left, right, preferred_element_type=jnp.float32)


def product_t(left, right):
    return lax.dot_general(
        left, right, (((1,), (1,)), ((), ())), preferred_element_type=jnp.float32
    )


def body(
    n,
    tokens,
    segment_ids,
    w_query,
    w_key,
    w_value,
    w_out,
    w_gate,
    w_up,
    w_down,
    gain_query,
    gain_key,
    gain_attn,
    gain_ffn,
    cotangent,
):
    width = w_query.shape[1]
    shards = jnp.stack(
        [
            jnp.concatenate([w_query, w_key, w_value, w_out.T], axis=1),
            w_gate,
            w_up,
            w_down.T,
        ]
    )
    gains = lax.all_gather(
        jnp.stack([gain_query, gain_key, gain_attn, gain_ffn]), "fsdp", axis=1, tiled=True
    ).astype(jnp.float32)
    D = gains.shape[1]
    rank = lax.axis_index("tensor")
    heads_here = width // HEAD_DIM
    start_col = rank * width
    rows = tokens.shape[0]
    length = 2 * rows
    segment_row = segment_ids[0]

    def arrange(row):
        return lax.dynamic_slice_in_dim(jnp.concatenate([row, row]), rank * rows, length)

    indices = arrange(jnp.arange(length, dtype=jnp.int32))
    positions = arrange(doc_positions(segment_row))
    segments = arrange(segment_row)
    cosine, sine_table = rope_tables(positions)
    allowed = (segments[:, None] == segments[None, :]) & (indices[:, None] >= indices[None, :])
    bias = jnp.where(allowed, 0.0, masked_score).astype(jnp.float32)
    (
        weights,
        layer_out,
        gathered,
        qk_hat,
        queries_r,
        keys_r,
        values,
        attended,
        attn_hat,
        middle_all,
        silu_gate,
        slope_gate,
        hidden,
        grad_down_all,
        factors,
        ffn_gain_grad,
    ) = forward(
        shards,
        tokens,
        cotangent,
        jnp.concatenate([gains, jnp.zeros_like(gains)]),
        jnp.concatenate([cosine, cosine], axis=1),
        jnp.concatenate([-sine_table, sine_table], axis=1),
        bias,
        n,
    )
    out_t = weights[0, :, 3 * width :]
    gate_full, up_full, down_t = weights[1], weights[2], weights[3]
    gain_query_here = lax.dynamic_slice_in_dim(gains[0], start_col, width)
    gain_key_here = lax.dynamic_slice_in_dim(gains[1], start_col, width)
    attn_gain_f = gains[2]
    ffn_gain_grad = ffn_gain_grad[0]
    query_hat, key_hat = qk_hat[:, :width], qk_hat[:, width:]
    query_factor, key_factor = factors[0, :, :1], factors[1, :, :1]
    attn_hat = attn_hat[:rows]
    attn_factor = factors[2, :rows, :1]
    queries_r = queries_r.reshape(length, heads_here, HEAD_DIM)
    keys_r = keys_r.reshape(length, heads_here, HEAD_DIM)
    values_r = values.reshape(length, heads_here, HEAD_DIM)
    grad_out = cotangent.astype(jnp.float32)
    grad_hidden = product(grad_down_all, down_t)
    grad_gate = (grad_hidden * slope_gate.astype(jnp.float32)).astype(jnp.bfloat16)
    grad_up = (grad_hidden * silu_gate.astype(jnp.float32)).astype(jnp.bfloat16)
    grad_middle = grad_out + reduce_rows(
        product_t(grad_gate, gate_full) + product_t(grad_up, up_full)
    )
    attn_gain_grad = jnp.sum(grad_middle * attn_hat, axis=0)
    grad_attn = norm_back(grad_middle, attn_hat, attn_factor, attn_gain_f).astype(jnp.bfloat16)
    grad_attn_all = both(grad_attn)
    grad_attended = (
        product(grad_attn_all, out_t).astype(jnp.bfloat16).reshape(length, heads_here, HEAD_DIM)
    )
    probs_again = jax.nn.softmax(attention_scores(queries_r, keys_r, allowed), axis=-1)
    grad_values = jnp.einsum(
        "hqk,qhd->khd",
        probs_again.astype(jnp.bfloat16),
        grad_attended,
        preferred_element_type=jnp.float32,
    ).astype(jnp.bfloat16)
    grad_probs = jnp.einsum(
        "qhd,khd->hqk", grad_attended, values_r, preferred_element_type=jnp.float32
    )
    grad_scores = (
        probs_again * (grad_probs - jnp.sum(probs_again * grad_probs, axis=-1, keepdims=True))
    ).astype(jnp.bfloat16)
    score_scale = HEAD_DIM ** (-0.5)
    grad_queries_r = (
        jnp.einsum("hqk,khd->qhd", grad_scores, keys_r, preferred_element_type=jnp.float32)
        * score_scale
    )
    grad_keys_r = (
        jnp.einsum("hqk,qhd->khd", grad_scores, queries_r, preferred_element_type=jnp.float32)
        * score_scale
    )
    grad_query_n = unrotate(grad_queries_r, cosine, sine_table).reshape(length, width)
    grad_key_n = unrotate(grad_keys_r, cosine, sine_table).reshape(length, width)
    query_gain_part = jnp.sum(grad_query_n * query_hat, axis=0)
    key_gain_part = jnp.sum(grad_key_n * key_hat, axis=0)
    query_scaled = grad_query_n * gain_query_here
    key_scaled = grad_key_n * gain_key_here
    dots = jnp.stack(
        [jnp.sum(query_scaled * query_hat, axis=1), jnp.sum(key_scaled * key_hat, axis=1)]
    )
    dots = dots + jnp.roll(lax.ppermute(dots, "tensor", SWAP), rows, axis=1)
    grad_queries = (query_factor * (query_scaled - query_hat * (dots[0] / D)[:, None])).astype(
        jnp.bfloat16
    )
    grad_keys = (key_factor * (key_scaled - key_hat * (dots[1] / D)[:, None])).astype(jnp.bfloat16)
    grad_values_flat = grad_values.reshape(length, width)
    grads_qkv = jnp.concatenate([grad_queries, grad_keys, grad_values_flat], axis=1)
    grad_input = grad_middle + reduce_rows(product_t(grads_qkv, weights[0, :, : 3 * width]))

    zeros = jnp.zeros((D,), jnp.float32)
    gain_parts = jnp.stack(
        [
            lax.dynamic_update_slice_in_dim(zeros, query_gain_part, start_col, 0),
            lax.dynamic_update_slice_in_dim(zeros, key_gain_part, start_col, 0),
            attn_gain_grad,
            ffn_gain_grad,
        ]
    )
    gain_sums = lax.psum(gain_parts, ("fsdp", "tensor"))
    share = D // (2 * n)
    gain_grads = lax.dynamic_slice_in_dim(gain_sums, lax.axis_index("fsdp") * share, share, axis=1)

    left = jnp.stack([grad_down_all.T, middle_all.T, gathered.T, grad_attn_all.T])
    right = jnp.stack(
        [hidden, grad_up, grad_gate, jnp.concatenate([grads_qkv, attended], axis=1)]
    )
    grads = scatter_gradients(left, right, n)
    first = grads[3]
    return (
        layer_out,
        grad_input,
        first[:, :width],
        first[:, width : 2 * width],
        first[:, 2 * width : 3 * width],
        first[:, 3 * width :].T,
        grads[2],
        grads[1],
        grads[0].T,
        gain_grads[0],
        gain_grads[1],
        gain_grads[2],
        gain_grads[3],
    )


def solution(mesh):
    rows, cols, gain = P("fsdp", "tensor"), P("tensor", "fsdp"), P("fsdp")
    acts = P(("fsdp", "tensor"), None)
    return jax.shard_map(
        functools.partial(body, mesh.shape["fsdp"] // 2),
        mesh=mesh,
        in_specs=(acts, P("fsdp", None), rows, rows, rows, cols, rows, rows, cols)
        + (gain,) * 4
        + (acts,),
        out_specs=(acts, acts, rows, rows, rows, cols, rows, rows, cols) + (gain,) * 4,
        check_vma=False,
    )
```
